32 devices in a mesh: ty: 16 (over z, y, core), tx: 2 (over x).
Axes of the slice: x: 2, y: 2, z: 4, core: 2. Of those that a mesh axis runs over, the one named last changes fastest.
Arguments:
- ctrl: float32 [16, 2, 512, 640], P('ty', 'tx'), may hold values from -6 to 6
- interp_wt: float32 [16, 2, 4, 128, 384], P('ty', 'tx'), may hold values from -0.3125 to 0.3125
- interp_cols: int32 [16, 2, 4, 384], P('ty', 'tx'), may hold values from 0 to 1023
- conv_wt: float32 [16, 2, 4, 128, 512], P('ty', 'tx'), may hold values from -0.25 to 0.25
- conv_cols: int32 [16, 2, 4, 512], P('ty', 'tx'), may hold values from 0 to 1023
- halo_index: int32 [16, 2, 8, 64], P('ty', 'tx'), may hold values from 0 to 511
- valid: int32 [16, 2], P('ty', 'tx'), may hold values from 256 to 512
Outputs:
- localized: float32 [16, 2, 512, 640], P('ty', 'tx')
The draws below stay inside these ranges and needn't reach their ends.
Inputs may be any that keep to these rules, and one draw needn't show every extreme that they name: `interp_cols`: indices into a tile's extended subgrid of 1024 rows; repeats are allowed. `conv_cols`: indices into a tile's extended subgrid; repeats are allowed. `halo_index`: owned row indices; repeats are allowed.
All inputs are finite; a program needn't handle non-finite values.
Results may differ from the reference program's by a relative error of at most 0.0001.
Values sent between devices are 32-bit elements; how exact they have to be, the bound alone decides.
No kernel may reach another device: no remote copies, remote signals or barrier semaphores. Data moves between devices by JAX's collectives and lax.ppermute only.
A program may use at most 64 MiB of HBM per device.

```python
import jax
import jax.numpy as jnp
from jax import lax

NODES = 512
GRID = 512
HALO = 64
GROWS = 128
GCOLS = 384
CROWS = 128
CCOLS = 512
FEAT = 640
EXT = 1024
GBLK = 4
CBLK = 4
N_TY = 16
N_TX = 2


def with_ends(array, key, smallest, top_value):
    longest = array.shape.index(max(array.shape))
    spots = []
    for shift in (0, 1):
        where = [jax.random.randint(jax.random.fold_in(key, axis), (), 0, length) for axis, length in enumerate(array.shape)]
        where[longest] = (where[longest] + shift) % array.shape[longest]
        spots.append(tuple(where))
    return array.at[spots[0]].set(smallest).at[spots[1]].set(top_value)


def steps_of(stream_key, dims, cuts, low, largest):
    gain, own = 1.0, jax.random.fold_in(stream_key, 6)
    for position, blocks in cuts:
        steps = jnp.exp(jax.random.uniform(jax.random.fold_in(own, position), (blocks,), jnp.float32, low / len(cuts), largest / len(cuts)))
        gain = gain * jnp.repeat(steps, dims[position] // blocks).reshape([-1 if axis == position else 1 for axis in range(len(dims))])
    return gain


def scatter_about(rng, shape, scale, most, cuts=(), kind=jnp.bfloat16):
    gain = steps_of(rng, shape, cuts, -0.22, 0.18) if cuts else 1.0
    values = jax.random.normal(rng, shape, jnp.float32) * scale * gain
    return jnp.minimum(jnp.maximum(values, -most), most).astype(kind)


def setup_inputs(seed: int = 0) -> dict:
    keys = jax.random.split(jax.random.key(seed), 8)
    return {
        "ctrl": scatter_about(keys[0], (N_TY, N_TX, GRID, FEAT), 1.0, 6.0, ((0, 16), (1, 2)), jnp.float32),
        "interp_wt": scatter_about(keys[1], (N_TY, N_TX, GBLK, GROWS, GCOLS), GCOLS ** -0.5, 0.3125, ((0, 16), (1, 2)), jnp.float32),
        "interp_cols": with_ends(jax.random.randint(keys[2], (N_TY, N_TX, GBLK, GCOLS), 0, EXT), jax.random.fold_in(keys[2], 1), 0, EXT - 1).astype(jnp.int32),
        "conv_wt": scatter_about(keys[3], (N_TY, N_TX, CBLK, CROWS, CCOLS), CCOLS ** -0.5, 0.25, ((0, 16), (1, 2)), jnp.float32),
        "conv_cols": with_ends(jax.random.randint(keys[4], (N_TY, N_TX, CBLK, CCOLS), 0, EXT), jax.random.fold_in(keys[4], 1), 0, EXT - 1).astype(jnp.int32),
        "halo_index": with_ends(jax.random.randint(keys[5], (N_TY, N_TX, 8, HALO), 0, NODES), jax.random.fold_in(keys[5], 1), 0, NODES - 1).astype(jnp.int32),
        "valid": with_ends(jax.random.randint(keys[6], (N_TY, N_TX), GRID // 2, GRID + 1), jax.random.fold_in(keys[6], 1), GRID // 2, GRID).astype(jnp.int32),
    }


DIRECTIONS = ((-1, -1), (-1, 0), (-1, 1), (0, -1), (0, 1), (1, -1), (1, 0), (1, 1))


def neighbour(tiles, row_off, col_off):
    shifted = jnp.roll(tiles, -col_off, axis=1)
    edge = jnp.zeros_like(shifted[:1])
    if row_off == 1:
        return jnp.concatenate([shifted[1:], edge], axis=0)
    if row_off == -1:
        return jnp.concatenate([edge, shifted[:-1]], axis=0)
    return shifted


def over_tiles(func, *arrays):
    rows_t, cols_t = arrays[0].shape[:2]
    flat = tuple(item.reshape((rows_t * cols_t,) + item.shape[2:]) for item in arrays)
    result = lax.map(lambda packed: func(*packed), flat)
    return result.reshape((rows_t, cols_t) + result.shape[1:])


def forward_blocks(weights, cols, source):
    gathered = jnp.take(source, cols, axis=0)
    result = jnp.einsum("bgc,bcf->bgf", weights, gathered, precision=lax.Precision.HIGHEST)
    return result.reshape(-1, source.shape[1])


def adjoint_blocks(weights, cols, values):
    blocks = values.reshape(weights.shape[0], weights.shape[1], values.shape[1])
    contrib = jnp.einsum("bgc,bgf->bcf", weights, blocks, precision=lax.Precision.HIGHEST)
    return jax.ops.segment_sum(contrib.reshape(-1, values.shape[1]), cols.reshape(-1), num_segments=EXT)


def accumulate(contrib, halo_index):
    owned = contrib[:, :, :NODES]
    slots = contrib[:, :, NODES:].reshape(contrib.shape[0], contrib.shape[1], 8, HALO, FEAT)
    for slot_id in range(8):
        row_off, col_off = DIRECTIONS[slot_id]
        arrived = neighbour(slots[:, :, slot_id], row_off, col_off)
        owned = owned + over_tiles(lambda vals, idx: jax.ops.segment_sum(vals, idx, num_segments=NODES), arrived, halo_index[:, :, slot_id])
    return owned


def extend(owned, halo_index):
    sends = over_tiles(lambda field, idx: jnp.take(field, idx, axis=0), owned, halo_index)
    slots = []
    for slot_id in range(8):
        row_off, col_off = DIRECTIONS[slot_id]
        slots.append(neighbour(sends[:, :, slot_id], -row_off, -col_off))
    stacked = jnp.stack(slots, axis=2).reshape(owned.shape[0], owned.shape[1], 8 * HALO, FEAT)
    return jnp.concatenate([owned, stacked], axis=2)


def reference(ctrl, interp_wt, interp_cols, conv_wt, conv_cols, halo_index, valid):
    positions = jnp.arange(GRID, dtype=jnp.int32)
    mask = (positions[None, None, :] < valid[:, :, None]).astype(jnp.float32)[..., None]
    masked = ctrl * mask
    a_ext = over_tiles(adjoint_blocks, interp_wt, interp_cols, masked)
    summed = accumulate(a_ext, halo_index)
    b_ext = over_tiles(adjoint_blocks, conv_wt, conv_cols, summed)
    spread = accumulate(b_ext, halo_index)
    smooth = over_tiles(forward_blocks, conv_wt, conv_cols, extend(spread, halo_index))
    result = over_tiles(forward_blocks, interp_wt, interp_cols, extend(smooth, halo_index))
    return result * mask
```

```python
import functools

import jax
import jax.numpy as jnp
from jax import lax
from jax.experimental import pallas as pl
from jax.experimental.pallas import tpu as pltpu
from jax.sharding import PartitionSpec as P

DIRECTIONS = ((-1, -1), (-1, 0), (-1, 1), (0, -1), (0, 1), (1, -1), (1, 0), (1, 1))
F32, BF16 = jnp.float32, jnp.bfloat16
VMEM = pl.BlockSpec(memory_space=pltpu.VMEM)
SMEM = pl.BlockSpec(memory_space=pltpu.SMEM)
PARAMS = pltpu.CompilerParams(vmem_limit_bytes=40 * 1024 * 1024)
TILE = 256


def split(x):
    high = x.astype(BF16)
    return high, (x - high.astype(F32)).astype(BF16)


def mul(left, right):
    return jnp.dot(left, right, preferred_element_type=F32)


def mul_nt(left, right):
    return lax.dot_general(left, right, (((1,), (1,)), ((), ())), preferred_element_type=F32)


def one_hot_t(row, count):
    ids = lax.broadcasted_iota(jnp.int32, (count, row.shape[1]), 0)
    return jnp.where(ids == row, 1.0, 0.0).astype(BF16)


def slot_groups(columns):
    groups = {}
    for slot, (row_off, col_off) in enumerate(DIRECTIONS):
        groups.setdefault((row_off, col_off % columns), []).append(slot)
    return [tuple(group) for group in groups.values()]


def exchange(pieces, groups, sign):
    rows_n, cols_n = lax.axis_size("ty"), lax.axis_size("tx")
    arrived = []
    for piece, group in zip(pieces, groups):
        row_off, col_off = (sign * step for step in DIRECTIONS[group[0]])
        pairs = [
            (i * cols_n + j, (i + row_off) * cols_n + (j + col_off) % cols_n)
            for i in range(rows_n)
            for j in range(cols_n)
            if 0 <= i + row_off < rows_n
        ]
        if row_off == 0 and col_off % cols_n == 0:
            arrived.append(piece)
        else:
            arrived.append(lax.ppermute(piece, ("ty", "tx"), pairs))
    return arrived


def place(refs, groups, halo):
    spots = {}
    for ref, group in zip(refs, groups):
        for k, slot in enumerate(group):
            spots[slot] = (ref, k * halo)
    return spots


def emit(block, start, own_ref, spots, own, halo):
    if start < own:
        own_ref[start : start + block.shape[0], :] = block
        return
    for at in range(0, block.shape[0], halo):
        ref, row = spots[(start - own + at) // halo]
        ref[row : row + halo, :] = block[at : at + halo]


def collect(spots, high_ref, low_ref, base, halo):
    for slot, (ref, row) in spots.items():
        high, low = split(ref[row : row + halo, :])
        at = base + slot * halo
        high_ref[at : at + halo, :] = high
        low_ref[at : at + halo, :] = low


def build_t(wt_ref, cols_ref, high_ref, low_ref):
    count = high_ref.shape[0]
    for b in range(wt_ref.shape[0]):
        size = wt_ref.shape[1]
        hot = one_hot_t(cols_ref[b : b + 1, :], count)
        both = mul_nt(hot, jnp.concatenate(split(wt_ref[b]), axis=0))
        high, low = split(both[:, :size] + both[:, size:])
        high_ref[:, b * size : (b + 1) * size] = high
        low_ref[:, b * size : (b + 1) * size] = low


def build(wt_ref, cols_ref, high_ref, low_ref):
    count = high_ref.shape[1]
    for b in range(wt_ref.shape[0]):
        size = wt_ref.shape[1]
        hot = one_hot_t(cols_ref[b : b + 1, :], count)
        both = mul_nt(jnp.concatenate(split(wt_ref[b]), axis=0), hot)
        high, low = split(both[:size] + both[size:])
        high_ref[b * size : (b + 1) * size, :] = high
        low_ref[b * size : (b + 1) * size, :] = low


def apply_t(high, low, mt_high, mt_low, own_ref, spots, own, halo):
    for start in range(0, mt_high.shape[0], TILE):
        rows = slice(start, start + TILE)
        block = mul(mt_high[rows, :], high) + mul(mt_high[rows, :], low) + mul(mt_low[rows, :], high)
        emit(block, start, own_ref, spots, own, halo)


def first_kernel(valid, ctrl, wt, cols, *refs, off, width, groups, own, halo, building):
    if building:
        own_out, *pieces, mt_high, mt_low = refs
        build_t(wt, cols, mt_high, mt_low)
    else:
        mt_high, mt_low = wt, cols
        own_out, *pieces = refs
    field = ctrl[0, 0, :, off : off + width]
    ids = lax.broadcasted_iota(jnp.int32, field.shape, 0)
    high, low = split(jnp.where(ids < valid[0, 0], field, 0.0))
    apply_t(high, low, mt_high, mt_low, own_out, place(pieces, groups, halo), own, halo)


def build_kernel(iwt, icols, cwt, ccols, halo_row, i_high, i_low, c_high, c_low, ct_high, ct_low, h_out, ht_out):
    build_t(cwt, ccols, ct_high, ct_low)
    build(cwt, ccols, c_high, c_low)
    build(iwt, icols, i_high, i_low)
    own = ht_out.shape[0]
    ids = lax.broadcasted_iota(jnp.int32, (own, halo_row.shape[1]), 0)
    hot = jnp.where(ids == halo_row[...], 1.0, 0.0)
    ht_out[...] = hot.astype(BF16)
    h_out[...] = hot.T.astype(BF16)


def owners(own_in, spots, ht, high_ref, low_ref, halo):
    collect(spots, high_ref, low_ref, 0, halo)
    return own_in[...] + mul(ht[...], high_ref[...]) + mul(ht[...], low_ref[...])


def second_kernel(own_in, *refs, groups, own, halo):
    n = len(groups)
    arrived, (ht, mt_high, mt_low, own_out), pieces, (s_high, s_low) = (
        refs[:n], refs[n : n + 4], refs[n + 4 : 2 * n + 4], refs[2 * n + 4 :])
    high, low = split(owners(own_in, place(arrived, groups, halo), ht, s_high, s_low, halo))
    apply_t(high, low, mt_high, mt_low, own_out, place(pieces, groups, halo), own, halo)


def send_rows(field, h, spots, own, halo):
    high, low = split(field)
    for start in range(0, h.shape[0], TILE):
        rows = slice(start, start + TILE)
        block = mul(h[rows, :], high) + mul(h[rows, :], low)
        emit(block, own + start, None, spots, own, halo)


def third_kernel(own_in, *refs, groups, own, halo):
    n = len(groups)
    arrived, (ht, h, own_out), pieces, (s_high, s_low) = (
        refs[:n], refs[n : n + 3], refs[n + 3 : 2 * n + 3], refs[2 * n + 3 :])
    total = owners(own_in, place(arrived, groups, halo), ht, s_high, s_low, halo)
    own_out[...] = total
    send_rows(total, h, place(pieces, groups, halo), own, halo)


def forward(own_in, arrived, groups, m_high, m_low, s_high, s_low, out, own, halo):
    high, low = split(own_in[...])
    s_high[0:own, :] = high
    s_low[0:own, :] = low
    collect(place(arrived, groups, halo), s_high, s_low, own, halo)
    for start in range(0, m_high.shape[0], TILE):
        rows = slice(start, start + TILE)
        out(rows, mul(m_high[rows, :], s_high[...]) + mul(m_high[rows, :], s_low[...])
            + mul(m_low[rows, :], s_high[...]))


def fourth_kernel(own_in, *refs, groups, own, halo):
    n = len(groups)
    arrived, (m_high, m_low, h, own_out), pieces, (s_high, s_low) = (
        refs[:n], refs[n : n + 4], refs[n + 4 : 2 * n + 4], refs[2 * n + 4 :])

    def store(rows, block):
        own_out[rows, :] = block

    forward(own_in, arrived, groups, m_high, m_low, s_high, s_low, store, own, halo)
    send_rows(own_out[...], h, place(pieces, groups, halo), own, halo)


def last_kernel(valid, own_in, *refs, groups, own, halo):
    n = len(groups)
    arrived, (m_high, m_low, own_out, s_high, s_low) = refs[:n], refs[n:]

    def store(rows, block):
        ids = lax.broadcasted_iota(jnp.int32, block.shape, 0) + rows.start
        own_out[rows, :] = jnp.where(ids < valid[0, 0], block, 0.0)

    forward(own_in, arrived, groups, m_high, m_low, s_high, s_low, store, own, halo)


def body(ctrl, interp_wt, interp_cols, conv_wt, conv_cols, halo_index, valid):
    iwt, icols = interp_wt[0, 0], interp_cols[0, 0]
    cwt, ccols = conv_wt[0, 0], conv_cols[0, 0]
    halo = halo_index.shape[3]
    halo_row = halo_index.reshape(1, -1)
    grid_rows, width_all = ctrl.shape[2:]
    own = cwt.shape[0] * cwt.shape[1]
    slots = halo_row.shape[1]
    ext = own + slots
    groups = slot_groups(lax.axis_size("tx"))
    known = dict(groups=groups, own=own, halo=halo)

    def shape(rows, cols, kind=F32):
        return jax.ShapeDtypeStruct((rows, cols), kind)

    def call(kernel, outs, args, scratch=(), smem=0, flops=0, **more):
        return pl.pallas_call(
            functools.partial(kernel, **more),
            out_shape=outs,
            in_specs=[SMEM] * smem + [VMEM] * (len(args) - smem),
            out_specs=jax.tree.map(lambda _: VMEM, outs),
            scratch_shapes=list(scratch),
            compiler_params=PARAMS,
            cost_estimate=pl.CostEstimate(flops=flops, transcendentals=0, bytes_accessed=4 << 20),
            name=kernel.__name__,
        )(*args)

    lanes = 128
    first = (width_all // (2 * lanes)) * lanes
    chunks = [(0, first), (first, width_all - first)] if first else [(0, width_all)]

    def pieces(width):
        return [shape(len(group) * halo, width) for group in groups]

    state = []
    for number, (off, width) in enumerate(chunks):
        outs = [shape(own, width)] + pieces(width)
        more = dict(off=off, width=width, building=number == 0, **known)
        if number == 0:
            outs += [shape(ext, grid_rows, BF16)] * 2
            *got, it_high, it_low = call(first_kernel, outs, (valid, ctrl, iwt, icols), smem=1, **more)
        else:
            got = call(first_kernel, outs, (valid, ctrl, it_high, it_low), smem=1, **more)
        state.append(got)
    operators = [shape(grid_rows, ext, BF16)] * 2 + [shape(own, ext, BF16)] * 2 + [shape(ext, own, BF16)] * 2
    i_high, i_low, c_high, c_low, ct_high, ct_low, h, ht = call(
        build_kernel, operators + [shape(slots, own, BF16), shape(own, slots, BF16)],
        (iwt, icols, cwt, ccols, halo_row))

    def scratch(rows, width):
        return [pltpu.VMEM((rows, width), BF16)] * 2

    def advance(sign, kernel, operands, rows):
        for number, (_, width) in enumerate(chunks):
            mine, *sent = state[number]
            arrived = exchange(sent, groups, sign)
            state[number] = call(kernel, [shape(own, width)] + pieces(width), (mine, *arrived, *operands),
                                 scratch(rows, width), **known)

    advance(-1, second_kernel, (ht, ct_high, ct_low), slots)
    advance(-1, third_kernel, (ht, h), slots)
    advance(1, fourth_kernel, (c_high, c_low, h), ext)
    results = []
    for number, (_, width) in enumerate(chunks):
        mine, *sent = state[number]
        arrived = exchange(sent, groups, 1)
        results.append(call(last_kernel, shape(grid_rows, width), (valid, mine, *arrived, i_high, i_low),
                            scratch(ext, width), smem=1, **known))
    return jnp.concatenate(results, axis=1)[None, None]


def solution(mesh):
    placed = (
        P("ty", "tx", None, None),
        P("ty", "tx", None, None, None),
        P("ty", "tx", None, None),
        P("ty", "tx", None, None, None),
        P("ty", "tx", None, None),
        P("ty", "tx", None, None),
        P("ty", "tx"),
    )
    return jax.shard_map(
        body, mesh=mesh, in_specs=placed, out_specs=P("ty", "tx", None, None), check_vma=False
    )
```

```python
import functools

import jax
import jax.numpy as jnp
from jax import lax
from jax.experimental import pallas as pl
from jax.experimental.pallas import tpu as pltpu
from jax.sharding import PartitionSpec as P


F32, BF16 = jnp.float32, jnp.bfloat16
VMEM = pl.BlockSpec(memory_space=pltpu.VMEM)
HBM = pl.BlockSpec(memory_space=pltpu.HBM)
SMEM = pl.BlockSpec(memory_space=pltpu.SMEM)
PARAMS = pltpu.CompilerParams(vmem_limit_bytes=40 * 1024 * 1024)
TILE = 256


def split(x):
    high = x.astype(BF16)
    return high, (x - high.astype(F32)).astype(BF16)


def mul(left, right):
    return jnp.dot(left, right, preferred_element_type=F32)


def mul_nt(left, right):
    return lax.dot_general(left, right, (((1,), (1,)), ((), ())), preferred_element_type=F32)


def one_hot_t(row, count):
    ids = lax.broadcasted_iota(jnp.int32, (count, row.shape[1]), 0)
    return jnp.where(ids == row, 1.0, 0.0).astype(BF16)


PLACES = ((None, -1), (None, 1), (0, -1), (0, 0), (0, 1), (1, -1), (1, 0), (1, 1))


def slot_groups(columns):
    groups = {}
    for place_id, (partner, step) in enumerate(PLACES):
        groups.setdefault((partner, step % columns), []).append(place_id)
    order = sorted(groups, key=lambda key: (key[1] == 0, {1: 0, 0: 1, None: 2}[key[0]]))
    return [tuple(groups[key]) for key in order]


def exchange(pieces, groups, sign):
    rows_n, cols_n = lax.axis_size("ty"), lax.axis_size("tx")
    arrived = []
    for piece, group in zip(pieces, groups):
        partner, step = PLACES[group[0]]
        pairs = []
        for i in range(rows_n):
            target = i if partner is None else ((i + partner) ^ 1) - partner
            if 0 <= target < rows_n:
                pairs += [(i * cols_n + j, target * cols_n + (j + sign * step) % cols_n) for j in range(cols_n)]
        if partner is None and step % cols_n == 0:
            arrived.append(piece)
        else:
            arrived.append(lax.ppermute(piece, ("ty", "tx"), pairs))
    return arrived


def relabelled(cols, odd, own, halo):
    above = jnp.where(odd, 5, 2)
    below = jnp.where(odd, -3, 0)
    moved = jnp.where(cols < own + 3 * halo, above, jnp.where(cols < own + 5 * halo, -3, below))
    return jnp.where(cols < own, cols, cols + moved * halo)


def place(refs, groups, halo):
    spots = {}
    for ref, group in zip(refs, groups):
        for k, slot in enumerate(group):
            spots[slot] = (ref, k * halo)
    return spots


def emit(block, start, own_ref, spots, own, halo):
    if start < own:
        own_ref[start : start + block.shape[0], :] = block
        return
    for at in range(0, block.shape[0], halo):
        ref, row = spots[(start - own + at) // halo]
        ref[row : row + halo, :] = block[at : at + halo]


def collect(spots, high_ref, low_ref, base, halo):
    for slot, (ref, row) in spots.items():
        high, low = split(ref[row : row + halo, :])
        at = base + slot * halo
        high_ref[at : at + halo, :] = high
        low_ref[at : at + halo, :] = low


def fetch(source, target, sems):
    copies = [pltpu.make_async_copy(source.at[0, 0, b], target.at[b], sems.at[b]) for b in range(target.shape[0])]
    for copy in copies:
        copy.start()
    return copies


def block_hot(cols_ref, b, count, order):
    return one_hot_t(relabelled(cols_ref[0, 0, b : b + 1, :], *order), count)


def build_t(wt_ref, copies, cols_ref, high_ref, low_ref, order):
    count = high_ref.shape[0]
    size = wt_ref.shape[1]
    for b in range(wt_ref.shape[0]):
        hot = block_hot(cols_ref, b, count, order)
        copies[b].wait()
        both = mul_nt(hot, jnp.concatenate(split(wt_ref[b]), axis=0))
        high, low = split(both[:, :size] + both[:, size:])
        high_ref[:, b * size : (b + 1) * size] = high
        low_ref[:, b * size : (b + 1) * size] = low


def build(wt_ref, cols_ref, high_ref, low_ref, order):
    count = high_ref.shape[1]
    size = wt_ref.shape[1]
    for b in range(wt_ref.shape[0]):
        both = mul_nt(jnp.concatenate(split(wt_ref[b]), axis=0), block_hot(cols_ref, b, count, order))
        high, low = split(both[:size] + both[size:])
        high_ref[b * size : (b + 1) * size, :] = high
        low_ref[b * size : (b + 1) * size, :] = low


def apply_t(high, low, mt_high, mt_low, own_ref, spots, own, halo):
    for start in range(0, mt_high.shape[0], TILE):
        rows = slice(start, start + TILE)
        block = mul(mt_high[rows, :], high) + mul(mt_high[rows, :], low) + mul(mt_low[rows, :], high)
        emit(block, start, own_ref, spots, own, halo)


def masked_apply(valid, field, mt_high, mt_low, own_out, pieces, groups, own, halo):
    ids = lax.broadcasted_iota(jnp.int32, field.shape, 0)
    high, low = split(jnp.where(ids < valid[0, 0], field, 0.0))
    apply_t(high, low, mt_high, mt_low, own_out, place(pieces, groups, halo), own, halo)


def first_kernel(valid, odd, ctrl, wt, cols, *refs, off, width, groups, own, halo):
    n = len(groups)
    (own_out, *pieces), (mt_high, mt_low, field, blocks, sem, sems) = refs[: n + 1], refs[n + 1 :]
    copies = fetch(wt, blocks, sems)
    copy = pltpu.make_async_copy(ctrl.at[0, 0, :, pl.ds(off, width)], field, sem)
    copy.start()
    build_t(blocks, copies, cols, mt_high, mt_low, (odd[0, 0] == 1, own, halo))
    copy.wait()
    masked_apply(valid, field[...], mt_high, mt_low, own_out, pieces, groups, own, halo)


def again_kernel(valid, ctrl, mt_high, mt_low, own_out, *refs, off, width, groups, own, halo):
    *pieces, field, sem = refs
    copy = pltpu.make_async_copy(ctrl.at[0, 0, :, pl.ds(off, width)], field, sem)
    copy.start()
    copy.wait()
    masked_apply(valid, field[...], mt_high, mt_low, own_out, pieces, groups, own, halo)


def build_kernel(odd, iwt, icols, cwt, ccols, halo_row, i_high, i_low, c_high, c_low, ct_high, ct_low, h_out, ht_out,
                 i_blocks, c_blocks, i_sems, c_sems, *, halo):
    own = ht_out.shape[0]
    order = (odd[0, 0] == 1, own, halo)
    c_copies = fetch(cwt, c_blocks, c_sems)
    i_copies = fetch(iwt, i_blocks, i_sems)
    ids = lax.broadcasted_iota(jnp.int32, (own, halo_row.shape[1]), 0)
    hot = jnp.where(ids == halo_row[...], 1.0, 0.0)
    ht_out[...] = hot.astype(BF16)
    h_out[...] = hot.T.astype(BF16)
    build_t(c_blocks, c_copies, ccols, ct_high, ct_low, order)
    build(c_blocks, ccols, c_high, c_low, order)
    for copy in i_copies:
        copy.wait()
    build(i_blocks, icols, i_high, i_low, order)


def owners(own_in, spots, ht, high_ref, low_ref, halo):
    collect(spots, high_ref, low_ref, 0, halo)
    return own_in[...] + mul(ht[...], high_ref[...]) + mul(ht[...], low_ref[...])


def second_kernel(own_in, *refs, groups, own, halo):
    n = len(groups)
    arrived, (ht, mt_high, mt_low, own_out), pieces, (s_high, s_low) = (
        refs[:n], refs[n : n + 4], refs[n + 4 : 2 * n + 4], refs[2 * n + 4 :])
    high, low = split(owners(own_in, place(arrived, groups, halo), ht, s_high, s_low, halo))
    apply_t(high, low, mt_high, mt_low, own_out, place(pieces, groups, halo), own, halo)


def send_rows(field, h, spots, own, halo):
    high, low = split(field)
    for start in range(0, h.shape[0], TILE):
        rows = slice(start, start + TILE)
        block = mul(h[rows, :], high) + mul(h[rows, :], low)
        emit(block, own + start, None, spots, own, halo)


def third_kernel(own_in, *refs, groups, own, halo):
    n = len(groups)
    arrived, (ht, h, own_out), pieces, (s_high, s_low) = (
        refs[:n], refs[n : n + 3], refs[n + 3 : 2 * n + 3], refs[2 * n + 3 :])
    total = owners(own_in, place(arrived, groups, halo), ht, s_high, s_low, halo)
    own_out[...] = total
    send_rows(total, h, place(pieces, groups, halo), own, halo)


def forward(own_in, arrived, groups, m_high, m_low, s_high, s_low, out, own, halo):
    high, low = split(own_in[...])
    s_high[0:own, :] = high
    s_low[0:own, :] = low
    collect(place(arrived, groups, halo), s_high, s_low, own, halo)
    for start in range(0, m_high.shape[0], TILE):
        rows = slice(start, start + TILE)
        out(rows, mul(m_high[rows, :], s_high[...]) + mul(m_high[rows, :], s_low[...])
            + mul(m_low[rows, :], s_high[...]))


def fourth_kernel(own_in, *refs, groups, own, halo):
    n = len(groups)
    arrived, (m_high, m_low, h, own_out), pieces, (s_high, s_low) = (
        refs[:n], refs[n : n + 4], refs[n + 4 : 2 * n + 4], refs[2 * n + 4 :])

    def store(rows, block):
        own_out[rows, :] = block

    forward(own_in, arrived, groups, m_high, m_low, s_high, s_low, store, own, halo)
    send_rows(own_out[...], h, place(pieces, groups, halo), own, halo)


def last_kernel(valid, own_in, *refs, groups, own, halo, off, width, chained):
    n = len(groups)
    arrived, (m_high, m_low, *rest) = refs[:n], refs[n:]
    out, s_high, s_low, result, sems = rest[1:] if chained else rest
    copies = []

    def store(rows, block):
        ids = lax.broadcasted_iota(jnp.int32, block.shape, 0) + rows.start
        result[rows, :] = jnp.where(ids < valid[0, 0], block, 0.0)
        copy = pltpu.make_async_copy(
            result.at[rows, :], out.at[0, 0, rows, pl.ds(off, width)], sems.at[rows.start // TILE])
        copy.start()
        copies.append(copy)

    forward(own_in, arrived, groups, m_high, m_low, s_high, s_low, store, own, halo)
    for copy in copies:
        copy.wait()


def body(ctrl, interp_wt, interp_cols, conv_wt, conv_cols, halo_index, valid):
    halo = halo_index.shape[3]
    grid_rows, width_all = ctrl.shape[2:]
    blocks, block_rows = conv_wt.shape[2:4]
    own = blocks * block_rows
    slots = 8 * halo
    ext = own + slots
    odd = lax.axis_index("ty") % 2
    index = halo_index[0, 0]
    up, down = index[0:3], index[5:8]
    halo_row = jnp.concatenate(
        [index[3:5], jnp.where(odd == 1, up, down), jnp.where(odd == 1, down, up)]).reshape(1, -1)
    odd = odd.astype(jnp.int32).reshape(1, 1)
    groups = slot_groups(lax.axis_size("tx"))
    known = dict(groups=groups, own=own, halo=halo)

    def shape(rows, cols, kind=F32):
        return jax.ShapeDtypeStruct((rows, cols), kind)

    def call(kernel, outs, args, specs, scratch=(), aliases=None, out_spec=VMEM, **more):
        return pl.pallas_call(
            functools.partial(kernel, **more),
            out_shape=outs,
            in_specs=list(specs) + [VMEM] * (len(args) - len(specs)),
            out_specs=jax.tree.map(lambda _: out_spec, outs),
            scratch_shapes=list(scratch),
            input_output_aliases=aliases or {},
            compiler_params=PARAMS,
            cost_estimate=pl.CostEstimate(flops=1 << 30, transcendentals=0, bytes_accessed=4 << 20),
        )(*args)

    lanes = 128
    second = (width_all // (2 * lanes)) * lanes
    chunks = [(0, width_all - second), (width_all - second, second)] if second else [(0, width_all)]
    dma = pltpu.SemaphoreType.DMA

    def leaving(width):
        return [shape(own, width)] + [shape(len(group) * halo, width) for group in groups]

    def weight_scratch(weights):
        return pltpu.VMEM(weights.shape[2:], F32), dma((weights.shape[2],))

    i_blocks, i_sems = weight_scratch(interp_wt)
    c_blocks, c_sems = weight_scratch(conv_wt)
    state = []
    for number, (off, width) in enumerate(chunks):
        more = dict(off=off, width=width, **known)
        field = pltpu.VMEM((grid_rows, width), F32)
        if number == 0:
            *got, it_high, it_low = call(
                first_kernel, leaving(width) + [shape(ext, grid_rows, BF16)] * 2,
                (valid, odd, ctrl, interp_wt, interp_cols), [SMEM, SMEM, HBM, HBM],
                [field, i_blocks, dma(()), i_sems], **more)
        else:
            got = call(again_kernel, leaving(width), (valid, ctrl, it_high, it_low), [SMEM, HBM],
                       [field, dma(())], **more)
        state.append(got)
    operators = [shape(grid_rows, ext, BF16)] * 2 + [shape(own, ext, BF16)] * 2 + [shape(ext, own, BF16)] * 2
    i_high, i_low, c_high, c_low, ct_high, ct_low, h, ht = call(
        build_kernel, operators + [shape(slots, own, BF16), shape(own, slots, BF16)],
        (odd, interp_wt, interp_cols, conv_wt, conv_cols, halo_row), [SMEM, HBM, VMEM, HBM],
        [i_blocks, c_blocks, i_sems, c_sems], halo=halo)

    def scratch(rows, width):
        return [pltpu.VMEM((rows, width), BF16)] * 2

    def arrive(number, sign):
        mine, *out = state[number]
        return mine, *exchange(out, groups, sign)

    def advance(sign, kernel, operands, rows):
        for number, (_, width) in enumerate(chunks):
            state[number] = call(kernel, leaving(width),
                                 (*arrive(number, sign), *operands), (), scratch(rows, width), **known)

    advance(-1, second_kernel, (ht, ct_high, ct_low), slots)
    advance(-1, third_kernel, (ht, h), slots)
    advance(1, fourth_kernel, (c_high, c_low, h), ext)
    result = None
    for number, (off, width) in enumerate(chunks):
        args = (valid, *arrive(number, 1), i_high, i_low)
        specs = [SMEM] + [VMEM] * (len(args) - 1)
        if number:
            args, specs = (*args, result), specs + [HBM]
        result = call(last_kernel, jax.ShapeDtypeStruct(ctrl.shape, F32), args, specs,
                      scratch(ext, width) + [pltpu.VMEM((grid_rows, width), F32), dma((grid_rows // TILE,))],
                      {len(args) - 1: 0} if number else None, HBM,
                      off=off, width=width, chained=number > 0, **known)
    return result


def solution(mesh):
    placed = (
        P("ty", "tx", None, None),
        P("ty", "tx", None, None, None),
        P("ty", "tx", None, None),
        P("ty", "tx", None, None, None),
        P("ty", "tx", None, None),
        P("ty", "tx", None, None),
        P("ty", "tx"),
    )

    return jax.shard_map(body, mesh=mesh, in_specs=placed, out_specs=P("ty", "tx", None, None), check_vma=False)
```

```python
import functools

import jax
import jax.numpy as jnp
from jax import lax
from jax.experimental import pallas as pl
from jax.experimental.pallas import tpu as pltpu
from jax.sharding import PartitionSpec as P


F32, BF16 = jnp.float32, jnp.bfloat16
VMEM = pl.BlockSpec(memory_space=pltpu.VMEM)
HBM = pl.BlockSpec(memory_space=pltpu.HBM)
SMEM = pl.BlockSpec(memory_space=pltpu.SMEM)
PARAMS = pltpu.CompilerParams(vmem_limit_bytes=24 * 1024 * 1024)
TILE = 256


def split(x):
    high = x.astype(BF16)
    return high, (x - high.astype(F32)).astype(BF16)


def mul(left, right):
    return jnp.dot(left, right, preferred_element_type=F32)


def mul_nt(left, right):
    return lax.dot_general(left, right, (((1,), (1,)), ((), ())), preferred_element_type=F32)


def one_hot_t(row, count):
    ids = lax.broadcasted_iota(jnp.int32, (count, row.shape[1]), 0)
    return jnp.where(ids == row, 1.0, 0.0).astype(BF16)


PLACES = ((None, -1), (None, 1), (0, -1), (0, 0), (0, 1), (1, -1), (1, 0), (1, 1))


def slot_groups(columns):
    groups = {}
    for place_id, (partner, step) in enumerate(PLACES):
        groups.setdefault((partner, step % columns), []).append(place_id)
    order = sorted(groups, key=lambda key: (key[1] == 0, {1: 0, 0: 1, None: 2}[key[0]]))
    return [tuple(groups[key]) for key in order]


def exchange(pieces, groups, sign):
    rows_n, cols_n = lax.axis_size("ty"), lax.axis_size("tx")
    arrived = []
    for piece, group in zip(pieces, groups):
        partner, step = PLACES[group[0]]
        pairs = []
        for i in range(rows_n):
            target = i if partner is None else ((i + partner) ^ 1) - partner
            if 0 <= target < rows_n:
                pairs += [(i * cols_n + j, target * cols_n + (j + sign * step) % cols_n) for j in range(cols_n)]
        if partner is None and step % cols_n == 0:
            arrived.append(piece)
        else:
            arrived.append(lax.ppermute(piece, ("ty", "tx"), pairs))
    return arrived


def relabelled(cols, odd, own, halo):
    above = jnp.where(odd, 5, 2)
    below = jnp.where(odd, -3, 0)
    moved = jnp.where(cols < own + 3 * halo, above, jnp.where(cols < own + 5 * halo, -3, below))
    return jnp.where(cols < own, cols, cols + moved * halo)


def place(refs, groups, halo):
    spots = {}
    for ref, group in zip(refs, groups):
        for k, slot in enumerate(group):
            spots[slot] = (ref, k * halo)
    return spots


def emit(block, start, own_ref, spots, own, halo):
    if start < own:
        own_ref[start : start + block.shape[0], :] = block
        return
    for at in range(0, block.shape[0], halo):
        ref, row = spots[(start - own + at) // halo]
        ref[row : row + halo, :] = block[at : at + halo]


def collect(spots, high_ref, low_ref, base, halo):
    for slot, (ref, row) in spots.items():
        high, low = split(ref[row : row + halo, :])
        at = base + slot * halo
        high_ref[at : at + halo, :] = high
        low_ref[at : at + halo, :] = low


def hot_blocks(cols, count, order):
    cols = relabelled(cols, *order)
    return [one_hot_t(cols[b : b + 1, :], count) for b in range(cols.shape[0])]


def build_t(wt_ref, hots, high_ref, low_ref):
    size = wt_ref.shape[-2]
    for b, hot in enumerate(hots):
        both = mul_nt(hot, jnp.concatenate(split(wt_ref[0, 0, b]), axis=0))
        high, low = split(both[:, :size] + both[:, size:])
        high_ref[:, b * size : (b + 1) * size] = high
        low_ref[:, b * size : (b + 1) * size] = low


def build(wt_ref, hots, high_ref, low_ref):
    size = wt_ref.shape[-2]
    for b, hot in enumerate(hots):
        both = mul_nt(jnp.concatenate(split(wt_ref[0, 0, b]), axis=0), hot)
        high, low = split(both[:size] + both[size:])
        high_ref[b * size : (b + 1) * size, :] = high
        low_ref[b * size : (b + 1) * size, :] = low


def apply_t(high, low, mt_high, mt_low, own_ref, spots, own, halo):
    for start in range(0, mt_high.shape[0], TILE):
        rows = slice(start, start + TILE)
        block = mul(mt_high[rows, :], high) + mul(mt_high[rows, :], low) + mul(mt_low[rows, :], high)
        emit(block, start, own_ref, spots, own, halo)


def masked_apply(valid, field, mt_high, mt_low, own_out, pieces, groups, own, halo):
    ids = lax.broadcasted_iota(jnp.int32, field.shape, 0)
    high, low = split(jnp.where(ids < valid[0, 0], field, 0.0))
    apply_t(high, low, mt_high, mt_low, own_out, place(pieces, groups, halo), own, halo)


def first_kernel(valid, odd, ctrl, wt, cols, *refs, off, width, groups, own, halo):
    n = len(groups)
    (own_out, *pieces), (mt_high, mt_low, field, blocks, cols_in, sems) = refs[: n + 1], refs[n + 1 :]
    copies = [
        pltpu.make_async_copy(cols, cols_in, sems.at[0]),
        pltpu.make_async_copy(wt, blocks, sems.at[1]),
        pltpu.make_async_copy(ctrl.at[0, 0, :, pl.ds(off, width)], field, sems.at[2]),
    ]
    for copy in copies:
        copy.start()
    copies[0].wait()
    hots = hot_blocks(cols_in[0, 0], mt_high.shape[0], (odd[0, 0] == 1, own, halo))
    copies[1].wait()
    build_t(blocks, hots, mt_high, mt_low)
    copies[2].wait()
    masked_apply(valid, field[...], mt_high, mt_low, own_out, pieces, groups, own, halo)


def again_kernel(valid, ctrl, mt_high, mt_low, own_out, *refs, off, width, groups, own, halo):
    *pieces, field, sem = refs
    copy = pltpu.make_async_copy(ctrl.at[0, 0, :, pl.ds(off, width)], field, sem)
    copy.start()
    copy.wait()
    masked_apply(valid, field[...], mt_high, mt_low, own_out, pieces, groups, own, halo)


def early_kernel(odd, wt, cols, halo_row, ct_high, ct_low, ht_out, *, halo):
    own = ht_out.shape[0]
    ht_out[...] = one_hot_t(halo_row[...], own)
    build_t(wt, hot_blocks(cols[0, 0], ct_high.shape[0], (odd[0, 0] == 1, own, halo)), ct_high, ct_low)


def conv_kernel(odd, wt, cols, ht, c_high, c_low, h_out, *, halo):
    h_out[...] = ht[...].astype(F32).T.astype(BF16)
    build(wt, hot_blocks(cols[0, 0], c_high.shape[1], (odd[0, 0] == 1, ht.shape[0], halo)), c_high, c_low)


def interp_kernel(odd, wt, cols, high, low, *, own, halo):
    build(wt, hot_blocks(cols[0, 0], high.shape[1], (odd[0, 0] == 1, own, halo)), high, low)


def owners(own_in, spots, ht, high_ref, low_ref, halo):
    collect(spots, high_ref, low_ref, 0, halo)
    return own_in[...] + mul(ht[...], high_ref[...]) + mul(ht[...], low_ref[...])


def second_kernel(own_in, *refs, groups, own, halo):
    n = len(groups)
    arrived, (ht, mt_high, mt_low, own_out), pieces, (s_high, s_low) = (
        refs[:n], refs[n : n + 4], refs[n + 4 : 2 * n + 4], refs[2 * n + 4 :])
    high, low = split(owners(own_in, place(arrived, groups, halo), ht, s_high, s_low, halo))
    apply_t(high, low, mt_high, mt_low, own_out, place(pieces, groups, halo), own, halo)


def send_rows(field, h, spots, own, halo):
    high, low = split(field)
    for start in range(0, h.shape[0], TILE):
        rows = slice(start, start + TILE)
        block = mul(h[rows, :], high) + mul(h[rows, :], low)
        emit(block, own + start, None, spots, own, halo)


def third_kernel(own_in, *refs, groups, own, halo):
    n = len(groups)
    arrived, (ht, h, own_out), pieces, (s_high, s_low) = (
        refs[:n], refs[n : n + 3], refs[n + 3 : 2 * n + 3], refs[2 * n + 3 :])
    total = owners(own_in, place(arrived, groups, halo), ht, s_high, s_low, halo)
    own_out[...] = total
    send_rows(total, h, place(pieces, groups, halo), own, halo)


def forward(own_in, arrived, groups, m_high, m_low, s_high, s_low, out, own, halo):
    high, low = split(own_in[...])
    s_high[0:own, :] = high
    s_low[0:own, :] = low
    collect(place(arrived, groups, halo), s_high, s_low, own, halo)
    for start in range(0, m_high.shape[0], TILE):
        rows = slice(start, start + TILE)
        out(rows, mul(m_high[rows, :], s_high[...]) + mul(m_high[rows, :], s_low[...])
            + mul(m_low[rows, :], s_high[...]))


def fourth_kernel(own_in, *refs, groups, own, halo):
    n = len(groups)
    arrived, (m_high, m_low, h, own_out), pieces, (s_high, s_low) = (
        refs[:n], refs[n : n + 4], refs[n + 4 : 2 * n + 4], refs[2 * n + 4 :])

    def store(rows, block):
        own_out[rows, :] = block

    forward(own_in, arrived, groups, m_high, m_low, s_high, s_low, store, own, halo)
    send_rows(own_out[...], h, place(pieces, groups, halo), own, halo)


def last_kernel(valid, own_in, *refs, groups, own, halo, off, width, chained):
    n = len(groups)
    arrived, (m_high, m_low, *rest) = refs[:n], refs[n:]
    out, s_high, s_low, result, sems = rest[1:] if chained else rest
    copies = []

    def store(rows, block):
        ids = lax.broadcasted_iota(jnp.int32, block.shape, 0) + rows.start
        result[rows, :] = jnp.where(ids < valid[0, 0], block, 0.0)
        copy = pltpu.make_async_copy(
            result.at[rows, :], out.at[0, 0, rows, pl.ds(off, width)], sems.at[rows.start // TILE])
        copy.start()
        copies.append(copy)

    forward(own_in, arrived, groups, m_high, m_low, s_high, s_low, store, own, halo)
    for copy in copies:
        copy.wait()


def body(ctrl, interp_wt, interp_cols, conv_wt, conv_cols, halo_index, valid):
    halo = halo_index.shape[3]
    grid_rows, width_all = ctrl.shape[2:]
    blocks, block_rows = conv_wt.shape[2:4]
    own = blocks * block_rows
    slots = 8 * halo
    ext = own + slots
    far_ctrl, far_wt, far_cols = (
        pltpu.with_memory_space_constraint(array, pltpu.HBM) for array in (ctrl, interp_wt, interp_cols))
    odd = lax.axis_index("ty") % 2
    index = halo_index[0, 0]
    up, down = index[0:3], index[5:8]
    halo_row = jnp.concatenate(
        [index[3:5], jnp.where(odd == 1, up, down), jnp.where(odd == 1, down, up)]).reshape(1, -1)
    odd = odd.astype(jnp.int32).reshape(1, 1)
    groups = slot_groups(lax.axis_size("tx"))
    known = dict(groups=groups, own=own, halo=halo)

    def shape(rows, cols, kind=F32):
        return jax.ShapeDtypeStruct((rows, cols), kind)

    def call(kernel, outs, args, specs, scratch=(), aliases=None, out_spec=VMEM, **more):
        return pl.pallas_call(
            functools.partial(kernel, **more),
            out_shape=outs,
            in_specs=list(specs) + [VMEM] * (len(args) - len(specs)),
            out_specs=jax.tree.map(lambda _: out_spec, outs),
            scratch_shapes=list(scratch),
            input_output_aliases=aliases or {},
            compiler_params=PARAMS,
            cost_estimate=pl.CostEstimate(flops=1 << 30, transcendentals=0, bytes_accessed=4 << 20),
        )(*args)

    lanes = 128
    second = (width_all // (2 * lanes)) * lanes
    chunks = [(0, width_all - second), (width_all - second, second)] if second else [(0, width_all)]
    dma = pltpu.SemaphoreType.DMA

    def leaving(width):
        return [shape(own, width)] + [shape(len(group) * halo, width) for group in groups]

    state = []
    for number, (off, width) in enumerate(chunks):
        more = dict(off=off, width=width, **known)
        field = pltpu.VMEM((grid_rows, width), F32)
        if number == 0:
            *got, it_high, it_low = call(
                first_kernel, leaving(width) + [shape(ext, grid_rows, BF16)] * 2,
                (valid, odd, far_ctrl, far_wt, far_cols), [SMEM, SMEM, HBM, HBM, HBM],
                [field, pltpu.VMEM(interp_wt.shape, F32), pltpu.VMEM(interp_cols.shape, jnp.int32), dma((3,))], **more)
        else:
            got = call(again_kernel, leaving(width), (valid, far_ctrl, it_high, it_low), [SMEM, HBM],
                       [field, dma(())], **more)
        state.append(got)
    ct_high, ct_low, ht = call(
        early_kernel, [shape(ext, own, BF16)] * 2 + [shape(own, slots, BF16)],
        (odd, conv_wt, conv_cols, halo_row), [SMEM], halo=halo)
    c_high, c_low, h = call(
        conv_kernel, [shape(own, ext, BF16)] * 2 + [shape(slots, own, BF16)],
        (odd, conv_wt, conv_cols, ht), [SMEM], halo=halo)
    i_high, i_low = call(
        interp_kernel, [shape(grid_rows, ext, BF16)] * 2, (odd, interp_wt, interp_cols), [SMEM],
        own=own, halo=halo)

    def scratch(rows, width):
        return [pltpu.VMEM((rows, width), BF16)] * 2

    def arrive(number, sign):
        mine, *out = state[number]
        return mine, *exchange(out, groups, sign)

    def advance(sign, kernel, operands, rows):
        for number, (_, width) in enumerate(chunks):
            state[number] = call(kernel, leaving(width),
                                 (*arrive(number, sign), *operands), (), scratch(rows, width), **known)

    advance(-1, second_kernel, (ht, ct_high, ct_low), slots)
    advance(-1, third_kernel, (ht, h), slots)
    advance(1, fourth_kernel, (c_high, c_low, h), ext)
    result = None
    for number, (off, width) in enumerate(chunks):
        args = (valid, *arrive(number, 1), i_high, i_low)
        specs = [SMEM] + [VMEM] * (len(args) - 1)
        if number:
            args, specs = (*args, result), specs + [HBM]
        result = call(last_kernel, jax.ShapeDtypeStruct(ctrl.shape, F32), args, specs,
                      scratch(ext, width) + [pltpu.VMEM((grid_rows, width), F32), dma((grid_rows // TILE,))],
                      {len(args) - 1: 0} if number else None, HBM,
                      off=off, width=width, chained=number > 0, **known)
    return result


def solution(mesh):
    placed = (
        P("ty", "tx", None, None),
        P("ty", "tx", None, None, None),
        P("ty", "tx", None, None),
        P("ty", "tx", None, None, None),
        P("ty", "tx", None, None),
        P("ty", "tx", None, None),
        P("ty", "tx"),
    )

    return jax.shard_map(body, mesh=mesh, in_specs=placed, out_specs=P("ty", "tx", None, None), check_vma=False)
```

```python
import functools

import jax
import jax.numpy as jnp
from jax import lax
from jax.experimental import pallas as pl
from jax.experimental.pallas import tpu as pltpu
from jax.sharding import PartitionSpec as P


F32, BF16 = jnp.float32, jnp.bfloat16
VMEM = pl.BlockSpec(memory_space=pltpu.VMEM)
HBM = pl.BlockSpec(memory_space=pltpu.HBM)
SMEM = pl.BlockSpec(memory_space=pltpu.SMEM)
PARAMS = pltpu.CompilerParams(vmem_limit_bytes=24 * 1024 * 1024)
TILE = 256


def split(x):
    high = x.astype(BF16)
    return high, (x - high.astype(F32)).astype(BF16)


def mul(left, right):
    return jnp.dot(left, right, preferred_element_type=F32)


def mul_nt(left, right):
    return lax.dot_general(left, right, (((1,), (1,)), ((), ())), preferred_element_type=F32)


def one_hot_t(row, count, low=0, high=0, gap=0):
    ids = lax.broadcasted_iota(jnp.int32, (count, row.shape[1]), 0) + low
    if gap:
        ids = jnp.where(ids < high, ids, ids + gap)
    return jnp.where(ids == row, 1.0, 0.0).astype(BF16)


PLACES = ((None, -1), (None, 1), (0, -1), (0, 1), (1, -1), (1, 1), (0, 0), (1, 0))
CROSSING = 6
FACING = {0: (3, 4, 0, 2, 5, 7, 1, 6), 1: (3, 4, 5, 7, 0, 2, 6, 1)}
TAKEN = {0: FACING[1], 1: FACING[0]}


def slot_groups(columns):
    groups = {}
    for place_id, (partner, step) in enumerate(PLACES):
        groups.setdefault((place_id < CROSSING, partner, step % columns), []).append(place_id)
    return [tuple(group) for group in groups.values()]


def exchange(pieces, groups, sign):
    rows_n, cols_n = lax.axis_size("ty"), lax.axis_size("tx")
    arrived = []
    for piece, group in zip(pieces, groups):
        partner, step = PLACES[group[0]]
        pairs = []
        for i in range(rows_n):
            target = i if partner is None else ((i + partner) ^ 1) - partner
            if 0 <= target < rows_n:
                pairs += [(i * cols_n + j, target * cols_n + (j + sign * step) % cols_n) for j in range(cols_n)]
        if partner is None and step % cols_n == 0:
            arrived.append(piece)
        else:
            arrived.append(lax.ppermute(piece, ("ty", "tx"), pairs))
    return arrived


def relabelled(cols, odd, own, halo):
    moved = jnp.zeros_like(cols)
    for slot in reversed(range(8)):
        shift = [(FACING[parity].index(slot) - slot) * halo for parity in (0, 1)]
        moved = jnp.where(cols < own + (slot + 1) * halo, jnp.where(odd, shift[1], shift[0]), moved)
    return jnp.where(cols < own, cols, cols + moved)


def place(refs, groups, halo):
    spots = {}
    for ref, group in zip(refs, groups):
        for k, slot in enumerate(group):
            spots[slot] = (ref, k * halo)
    return spots


def emit(block, start, own_ref, spots, own, halo):
    if start < own:
        own_ref[start : start + block.shape[0], :] = block
        return
    for at in range(0, block.shape[0], halo):
        ref, row = spots[(start - own + at) // halo]
        ref[row : row + halo, :] = block[at : at + halo]


def collect(spots, high_ref, low_ref, base, halo):
    for slot, (ref, row) in spots.items():
        high, low = split(ref[row : row + halo, :])
        at = base + slot * halo
        high_ref[at : at + halo, :] = high
        low_ref[at : at + halo, :] = low


def hot_blocks(cols, count, order, **rows):
    cols = relabelled(cols, *order)
    return [one_hot_t(cols[b : b + 1, :], count, **rows) for b in range(cols.shape[0])]


def build_t(wt_ref, hots, high_ref, low_ref):
    size = wt_ref.shape[-2]
    for b, hot in enumerate(hots):
        both = mul_nt(hot, jnp.concatenate(split(wt_ref[0, 0, b]), axis=0))
        high, low = split(both[:, :size] + both[:, size:])
        high_ref[:, b * size : (b + 1) * size] = high
        low_ref[:, b * size : (b + 1) * size] = low


def build(wt_ref, hots, high_ref, low_ref):
    size = wt_ref.shape[-2]
    for b, hot in enumerate(hots):
        both = mul_nt(jnp.concatenate(split(wt_ref[0, 0, b]), axis=0), hot)
        high, low = split(both[:size] + both[size:])
        high_ref[b * size : (b + 1) * size, :] = high
        low_ref[b * size : (b + 1) * size, :] = low


def apply_t(high, low, mt_high, mt_low, own_ref, spots, own, halo, base=0, first=0, last=None):
    last = mt_high.shape[0] if last is None else last
    for start in range(first, last, TILE):
        rows = slice(start, min(start + TILE, last))
        block = mul(mt_high[rows, :], high) + mul(mt_high[rows, :], low) + mul(mt_low[rows, :], high)
        emit(block, start - first + base, own_ref, spots, own, halo)


def first_kernel(valid, odd, ctrl, wt, cols, *refs, chunks, groups, own, halo, crossing):
    n = len(groups)
    each = n if crossing else n + 1
    outs, (mt_high, mt_low, field, blocks, cols_in, sems) = refs[: each * len(chunks)], refs[each * len(chunks) :]
    copies = [
        pltpu.make_async_copy(cols, cols_in, sems.at[0]),
        pltpu.make_async_copy(wt, blocks, sems.at[1]),
        pltpu.make_async_copy(ctrl, field, sems.at[2]),
    ]
    for copy in copies:
        copy.start()
    copies[0].wait()
    side = CROSSING * halo
    rows = dict(low=own) if crossing else dict(high=own, gap=side)
    hots = hot_blocks(cols_in[0, 0], mt_high.shape[0], (odd[0, 0] == 1, own, halo), **rows)
    copies[1].wait()
    build_t(blocks, hots, mt_high, mt_low)
    copies[2].wait()
    for number, (off, width) in enumerate(chunks):
        mine = outs[number * each : (number + 1) * each]
        part = field[0, 0, :, off : off + width]
        ids = lax.broadcasted_iota(jnp.int32, part.shape, 0)
        high, low = split(jnp.where(ids < valid[0, 0], part, 0.0))
        if crossing:
            apply_t(high, low, mt_high, mt_low, None, place(mine, groups, halo), own, halo, base=own)
        else:
            spots = place(mine[1:], groups, halo)
            apply_t(high, low, mt_high, mt_low, mine[0], spots, own, halo, last=own)
            apply_t(high, low, mt_high, mt_low, mine[0], spots, own, halo, base=own + side, first=own)


def early_kernel(odd, wt, cols, index, ct_high, ct_low, ht_out, *, halo):
    own = ht_out.shape[0]
    turned = odd[0, 0] == 1
    for at, (even_slot, odd_slot) in enumerate(zip(TAKEN[0], TAKEN[1])):
        row = jnp.where(turned, index[0, 0, odd_slot : odd_slot + 1, :], index[0, 0, even_slot : even_slot + 1, :])
        ht_out[:, at * halo : (at + 1) * halo] = one_hot_t(row, own)
    build_t(wt, hot_blocks(cols[0, 0], ct_high.shape[0], (turned, own, halo)), ct_high, ct_low)


def conv_kernel(odd, wt, cols, ht, c_high, c_low, h_out, *, halo):
    h_out[...] = ht[...].astype(F32).T.astype(BF16)
    build(wt, hot_blocks(cols[0, 0], c_high.shape[1], (odd[0, 0] == 1, ht.shape[0], halo)), c_high, c_low)


def interp_kernel(odd, wt, cols, high, low, *, own, halo):
    build(wt, hot_blocks(cols[0, 0], high.shape[1], (odd[0, 0] == 1, own, halo)), high, low)


def owners(own_in, spots, ht, high_ref, low_ref, halo):
    collect(spots, high_ref, low_ref, 0, halo)
    return own_in[...] + mul(ht[...], high_ref[...]) + mul(ht[...], low_ref[...])


def second_kernel(own_in, *refs, groups, own, halo):
    n = len(groups)
    arrived, (ht, mt_high, mt_low, own_out), pieces, (s_high, s_low) = (
        refs[:n], refs[n : n + 4], refs[n + 4 : 2 * n + 4], refs[2 * n + 4 :])
    high, low = split(owners(own_in, place(arrived, groups, halo), ht, s_high, s_low, halo))
    apply_t(high, low, mt_high, mt_low, own_out, place(pieces, groups, halo), own, halo)


def send_rows(field, h, spots, own, halo):
    high, low = split(field)
    for start in range(0, h.shape[0], TILE):
        rows = slice(start, start + TILE)
        block = mul(h[rows, :], high) + mul(h[rows, :], low)
        emit(block, own + start, None, spots, own, halo)


def third_kernel(own_in, *refs, groups, own, halo):
    n = len(groups)
    arrived, (ht, h, own_out), pieces, (s_high, s_low) = (
        refs[:n], refs[n : n + 3], refs[n + 3 : 2 * n + 3], refs[2 * n + 3 :])
    total = owners(own_in, place(arrived, groups, halo), ht, s_high, s_low, halo)
    own_out[...] = total
    send_rows(total, h, place(pieces, groups, halo), own, halo)


def forward(own_in, arrived, groups, m_high, m_low, s_high, s_low, out, own, halo):
    high, low = split(own_in[...])
    s_high[0:own, :] = high
    s_low[0:own, :] = low
    collect(place(arrived, groups, halo), s_high, s_low, own, halo)
    for start in range(0, m_high.shape[0], TILE):
        rows = slice(start, start + TILE)
        out(rows, mul(m_high[rows, :], s_high[...]) + mul(m_high[rows, :], s_low[...])
            + mul(m_low[rows, :], s_high[...]))


def fourth_kernel(own_in, *refs, groups, own, halo):
    n = len(groups)
    arrived, (m_high, m_low, h, own_out), pieces, (s_high, s_low) = (
        refs[:n], refs[n : n + 4], refs[n + 4 : 2 * n + 4], refs[2 * n + 4 :])

    def store(rows, block):
        own_out[rows, :] = block

    forward(own_in, arrived, groups, m_high, m_low, s_high, s_low, store, own, halo)
    send_rows(own_out[...], h, place(pieces, groups, halo), own, halo)


def last_kernel(valid, own_in, *refs, groups, own, halo, off, width):
    n = len(groups)
    arrived, (m_high, m_low, out, s_high, s_low, result, sems) = refs[:n], refs[n:]
    copies = []

    def store(rows, block):
        copies.append(write_rows(valid, block, rows, result, out, off, width, sems))

    forward(own_in, arrived, groups, m_high, m_low, s_high, s_low, store, own, halo)
    for copy in copies:
        copy.wait()


def write_rows(valid, block, rows, result, out, off, width, sems):
    ids = lax.broadcasted_iota(jnp.int32, block.shape, 0) + rows.start
    result[rows, :] = jnp.where(ids < valid[0, 0], block, 0.0)
    copy = pltpu.make_async_copy(result.at[rows, :], out.at[0, 0, rows, pl.ds(off, width)], sems.at[rows.start // TILE])
    copy.start()
    return copy


def part_kernel(own_in, *refs, groups, own, halo):
    n = len(groups) - 1
    arrived, (m_high, m_low, out, s_high, s_low) = refs[:n], refs[n:]
    count = len(groups[0]) * halo
    for ref in (s_high, s_low):
        ref[own : own + count, :] = jnp.zeros((count, ref.shape[1]), BF16)

    def store(rows, block):
        out[rows, :] = block

    forward(own_in, arrived, groups[1:], m_high, m_low, s_high, s_low, store, own, halo)


def tail_kernel(valid, part, late, m_high, m_low, so_far, out, result, sems, *, own, off, width):
    del so_far
    high, low = split(late[...])
    cols = slice(own, own + late.shape[0])
    copies = []
    for start in range(0, m_high.shape[0], TILE):
        rows = slice(start, start + TILE)
        block = (mul(m_high[rows, cols], high) + mul(m_high[rows, cols], low)
                 + mul(m_low[rows, cols], high) + part[rows, :])
        copies.append(write_rows(valid, block, rows, result, out, off, width, sems))
    for copy in copies:
        copy.wait()


def body(ctrl, interp_wt, interp_cols, conv_wt, conv_cols, halo_index, valid):
    halo = halo_index.shape[3]
    grid_rows, width_all = ctrl.shape[2:]
    blocks, block_rows = conv_wt.shape[2:4]
    own = blocks * block_rows
    slots = 8 * halo
    ext = own + slots
    far_ctrl, far_wt, far_cols = (
        pltpu.with_memory_space_constraint(array, pltpu.HBM) for array in (ctrl, interp_wt, interp_cols))
    odd = lax.axis_index("ty") % 2
    odd = odd.astype(jnp.int32).reshape(1, 1)
    groups = slot_groups(lax.axis_size("tx"))
    known = dict(groups=groups, own=own, halo=halo)

    def shape(rows, cols, kind=F32):
        return jax.ShapeDtypeStruct((rows, cols), kind)

    def call(kernel, outs, args, specs, scratch=(), aliases=None, out_spec=VMEM, **more):
        return pl.pallas_call(
            functools.partial(kernel, **more),
            out_shape=outs,
            in_specs=list(specs) + [VMEM] * (len(args) - len(specs)),
            out_specs=jax.tree.map(lambda _: out_spec, outs),
            scratch_shapes=list(scratch),
            input_output_aliases=aliases or {},
            compiler_params=PARAMS,
            cost_estimate=pl.CostEstimate(flops=1 << 30, transcendentals=0, bytes_accessed=4 << 20),
        )(*args)

    lanes = 128
    second = (width_all // (2 * lanes)) * lanes
    chunks = [(0, width_all - second), (width_all - second, second)] if second else [(0, width_all)]
    dma = pltpu.SemaphoreType.DMA

    def leaving(width):
        return [shape(own, width)] + [shape(len(group) * halo, width) for group in groups]

    crossing = [group for group in groups if group[0] < CROSSING]
    straight = groups[len(crossing) :]

    def first(kind, count):
        shapes = []
        for _, width in chunks:
            shapes += [] if kind else [shape(own, width)]
            shapes += [shape(len(group) * halo, width) for group in (crossing if kind else straight)]
        outs = call(
            first_kernel, shapes, (valid, odd, far_ctrl, far_wt, far_cols), [SMEM, SMEM, HBM, HBM, HBM],
            [pltpu.VMEM((count, grid_rows), BF16)] * 2
            + [pltpu.VMEM(ctrl.shape, F32), pltpu.VMEM(interp_wt.shape, F32), pltpu.VMEM(interp_cols.shape, jnp.int32),
               dma((3,))],
            chunks=chunks, groups=crossing if kind else straight, own=own, halo=halo, crossing=kind)
        each = len(outs) // len(chunks)
        return [list(outs[k * each : (k + 1) * each]) for k in range(len(chunks))]

    over = first(True, CROSSING * halo)
    rest = first(False, ext - CROSSING * halo)
    state = [[mine[0]] + sent + mine[1:] for sent, mine in zip(over, rest)]
    ct_high, ct_low, ht = call(
        early_kernel, [shape(ext, own, BF16)] * 2 + [shape(own, slots, BF16)],
        (odd, conv_wt, conv_cols, halo_index), [SMEM], halo=halo)
    c_high, c_low, h = call(
        conv_kernel, [shape(own, ext, BF16)] * 2 + [shape(slots, own, BF16)],
        (odd, conv_wt, conv_cols, ht), [SMEM], halo=halo)
    i_high, i_low = call(
        interp_kernel, [shape(grid_rows, ext, BF16)] * 2, (odd, interp_wt, interp_cols), [SMEM],
        own=own, halo=halo)

    def scratch(rows, width):
        return [pltpu.VMEM((rows, width), BF16)] * 2

    def arrive(number, sign):
        mine, *out = state[number]
        return mine, *exchange(out, groups, sign)

    def advance(sign, kernel, operands, rows):
        for number, (_, width) in enumerate(chunks):
            state[number] = call(kernel, leaving(width),
                                 (*arrive(number, sign), *operands), (), scratch(rows, width), **known)

    advance(-1, second_kernel, (ht, ct_high, ct_low), slots)
    advance(-1, third_kernel, (ht, h), slots)
    advance(1, fourth_kernel, (c_high, c_low, h), ext)
    whole = jax.ShapeDtypeStruct(ctrl.shape, F32)
    result = None
    for number, (off, width) in enumerate(chunks):
        mine, *arrived = arrive(number, 1)
        final = [pltpu.VMEM((grid_rows, width), F32), dma((grid_rows // TILE,))]
        if number == 0:
            result = call(last_kernel, whole, (valid, mine, *arrived, i_high, i_low), [SMEM],
                          scratch(ext, width) + final, None, HBM, off=off, width=width, **known)
        else:
            part = call(part_kernel, shape(grid_rows, width), (mine, *arrived[1:], i_high, i_low), (),
                        scratch(ext, width), **known)
            args = (valid, part, arrived[0], i_high, i_low, result)
            result = call(tail_kernel, whole, args, [SMEM] + [VMEM] * 4 + [HBM], final, {5: 0}, HBM,
                          own=own, off=off, width=width)
    return result


def solution(mesh):
    placed = (
        P("ty", "tx", None, None),
        P("ty", "tx", None, None, None),
        P("ty", "tx", None, None),
        P("ty", "tx", None, None, None),
        P("ty", "tx", None, None),
        P("ty", "tx", None, None),
        P("ty", "tx"),
    )

    return jax.shard_map(body, mesh=mesh, in_specs=placed, out_specs=P("ty", "tx", None, None), check_vma=False)
```

```python
import functools

import jax
import jax.numpy as jnp
from jax import lax
from jax.experimental import pallas as pl
from jax.experimental.pallas import tpu as pltpu
from jax.sharding import PartitionSpec as P


F32, BF16 = jnp.float32, jnp.bfloat16
VMEM = pl.BlockSpec(memory_space=pltpu.VMEM)
HBM = pl.BlockSpec(memory_space=pltpu.HBM)
SMEM = pl.BlockSpec(memory_space=pltpu.SMEM)
PARAMS = pltpu.CompilerParams(vmem_limit_bytes=24 * 1024 * 1024)
TILE = 256


def split(x):
    high = x.astype(BF16)
    return high, (x - high.astype(F32)).astype(BF16)


def mul(left, right):
    return jnp.dot(left, right, preferred_element_type=F32)


def mul_split(m_high, m_low, high, low):
    width = high.shape[1]
    both = mul(m_high, jnp.concatenate([high, low], axis=1))
    return both[:, :width] + both[:, width:] + mul(m_low, high)


def mul_nt(left, right):
    return lax.dot_general(left, right, (((1,), (1,)), ((), ())), preferred_element_type=F32)


def one_hot_t(row, count, low=0, high=0, gap=0):
    ids = lax.broadcasted_iota(jnp.int32, (count, row.shape[1]), 0) + low
    if gap:
        ids = jnp.where(ids < high, ids, ids + gap)
    return jnp.where(ids == row, 1.0, 0.0).astype(BF16)


PLACES = ((None, -1), (None, 1), (0, -1), (0, 1), (1, -1), (1, 1), (0, 0), (1, 0))
CROSSING = 6
FACING = {0: (3, 4, 0, 2, 5, 7, 1, 6), 1: (3, 4, 5, 7, 0, 2, 6, 1)}
TAKEN = {0: FACING[1], 1: FACING[0]}


def slot_groups(columns):
    groups = {}
    for place_id, (partner, step) in enumerate(PLACES):
        groups.setdefault((place_id < CROSSING, partner, step % columns), []).append(place_id)
    return [tuple(group) for group in groups.values()]


def exchange(pieces, groups, sign):
    rows_n, cols_n = lax.axis_size("ty"), lax.axis_size("tx")
    arrived = []
    for piece, group in zip(pieces, groups):
        partner, step = PLACES[group[0]]
        pairs = []
        for i in range(rows_n):
            target = i if partner is None else ((i + partner) ^ 1) - partner
            if 0 <= target < rows_n:
                pairs += [(i * cols_n + j, target * cols_n + (j + sign * step) % cols_n) for j in range(cols_n)]
        if partner is None and step % cols_n == 0:
            arrived.append(piece)
        else:
            arrived.append(lax.ppermute(piece, ("ty", "tx"), pairs))
    return arrived


def relabelled(cols, odd, own, halo):
    moved = jnp.zeros_like(cols)
    for slot in reversed(range(8)):
        shift = [(FACING[parity].index(slot) - slot) * halo for parity in (0, 1)]
        moved = jnp.where(cols < own + (slot + 1) * halo, jnp.where(odd, shift[1], shift[0]), moved)
    return jnp.where(cols < own, cols, cols + moved)


def place(refs, groups, halo):
    spots = {}
    for ref, group in zip(refs, groups):
        for k, slot in enumerate(group):
            spots[slot] = (ref, k * halo)
    return spots


def emit(block, start, own_ref, spots, own, halo):
    if start < own:
        own_ref[start : start + block.shape[0], :] = block
        return
    for at in range(0, block.shape[0], halo):
        ref, row = spots[(start - own + at) // halo]
        ref[row : row + halo, :] = block[at : at + halo]


def collect(spots, high_ref, low_ref, base, halo):
    for slot, (ref, row) in spots.items():
        high, low = split(ref[row : row + halo, :])
        at = base + slot * halo
        high_ref[at : at + halo, :] = high
        low_ref[at : at + halo, :] = low


def hot_blocks(cols, count, order, **rows):
    cols = relabelled(cols, *order)
    return [one_hot_t(cols[b : b + 1, :], count, **rows) for b in range(cols.shape[0])]


def build_t(wt_ref, hots, high_ref, low_ref):
    size = wt_ref.shape[-2]
    for b, hot in enumerate(hots):
        both = mul_nt(hot, jnp.concatenate(split(wt_ref[0, 0, b]), axis=0))
        high, low = split(both[:, :size] + both[:, size:])
        high_ref[:, b * size : (b + 1) * size] = high
        low_ref[:, b * size : (b + 1) * size] = low


def build(wt_ref, hots, high_ref, low_ref):
    size = wt_ref.shape[-2]
    for b, hot in enumerate(hots):
        both = mul_nt(jnp.concatenate(split(wt_ref[0, 0, b]), axis=0), hot)
        high, low = split(both[:size] + both[size:])
        high_ref[b * size : (b + 1) * size, :] = high
        low_ref[b * size : (b + 1) * size, :] = low


def apply_t(high, low, mt_high, mt_low, own_ref, spots, own, halo, base=0, first=0, last=None):
    last = mt_high.shape[0] if last is None else last
    for start in range(first, last, TILE):
        rows = slice(start, min(start + TILE, last))
        block = mul_split(mt_high[rows, :], mt_low[rows, :], high, low)
        emit(block, start - first + base, own_ref, spots, own, halo)


def first_kernel(valid, odd, ctrl, wt, cols, high, low, blocks, cols_in, *refs, chunks, groups, own, halo):
    n = len(groups)
    outs, (mt_high, mt_low, field, sems) = refs[: n * len(chunks)], refs[n * len(chunks) :]
    copies = [
        pltpu.make_async_copy(cols, cols_in, sems.at[0]),
        pltpu.make_async_copy(wt, blocks, sems.at[1]),
        pltpu.make_async_copy(ctrl, field, sems.at[2]),
    ]
    for copy in copies:
        copy.start()
    copies[0].wait()
    hots = hot_blocks(cols_in[0, 0], mt_high.shape[0], (odd[0, 0] == 1, own, halo), low=own)
    copies[1].wait()
    build_t(blocks, hots, mt_high, mt_low)
    copies[2].wait()
    ids = lax.broadcasted_iota(jnp.int32, high.shape, 0)
    high[...], low[...] = split(jnp.where(ids < valid[0, 0], field[0, 0], 0.0))
    for number, (off, width) in enumerate(chunks):
        spots = place(outs[number * n : (number + 1) * n], groups, halo)
        cols_of = slice(off, off + width)
        apply_t(high[:, cols_of], low[:, cols_of], mt_high, mt_low, None, spots, own, halo, base=own)


def rest_kernel(odd, high, low, wt, cols, *refs, chunks, groups, own, halo):
    each = len(groups) + 1
    outs, (mt_high, mt_low) = refs[: each * len(chunks)], refs[each * len(chunks) :]
    side = CROSSING * halo
    build_t(wt, hot_blocks(cols[0, 0], mt_high.shape[0], (odd[0, 0] == 1, own, halo), high=own, gap=side), mt_high, mt_low)
    for number, (off, width) in enumerate(chunks):
        mine = outs[number * each : (number + 1) * each]
        part = high[:, off : off + width], low[:, off : off + width]
        spots = place(mine[1:], groups, halo)
        apply_t(*part, mt_high, mt_low, mine[0], spots, own, halo, last=own)
        apply_t(*part, mt_high, mt_low, mine[0], spots, own, halo, base=own + side, first=own)


def early_kernel(odd, wt, cols, index, ct_high, ct_low, ht_out, h_out, *, halo):
    own = ht_out.shape[0]
    turned = odd[0, 0] == 1
    for at, (even_slot, odd_slot) in enumerate(zip(TAKEN[0], TAKEN[1])):
        row = jnp.where(turned, index[0, 0, odd_slot : odd_slot + 1, :], index[0, 0, even_slot : even_slot + 1, :])
        hot = one_hot_t(row, own)
        ht_out[:, at * halo : (at + 1) * halo] = hot
        h_out[at * halo : (at + 1) * halo, :] = hot.astype(F32).T.astype(BF16)
    build_t(wt, hot_blocks(cols[0, 0], ct_high.shape[0], (turned, own, halo)), ct_high, ct_low)


def late_kernel(odd, wt, cols, high, low, *, own, halo):
    build(wt, hot_blocks(cols[0, 0], high.shape[1], (odd[0, 0] == 1, own, halo)), high, low)


def owners(own_in, spots, ht, high_ref, low_ref, halo):
    collect(spots, high_ref, low_ref, 0, halo)
    return own_in[...] + mul(ht[...], high_ref[...]) + mul(ht[...], low_ref[...])


def second_kernel(own_in, *refs, groups, own, halo):
    n = len(groups)
    arrived, (ht, mt_high, mt_low, own_out), pieces, (s_high, s_low) = (
        refs[:n], refs[n : n + 4], refs[n + 4 : 2 * n + 4], refs[2 * n + 4 :])
    high, low = split(owners(own_in, place(arrived, groups, halo), ht, s_high, s_low, halo))
    apply_t(high, low, mt_high, mt_low, own_out, place(pieces, groups, halo), own, halo)


def send_rows(field, h, spots, own, halo):
    high, low = split(field)
    for start in range(0, h.shape[0], TILE):
        rows = slice(start, start + TILE)
        block = mul(h[rows, :], high) + mul(h[rows, :], low)
        emit(block, own + start, None, spots, own, halo)


def third_kernel(own_in, *refs, groups, own, halo):
    n = len(groups)
    arrived, (ht, h, own_out), pieces, (s_high, s_low) = (
        refs[:n], refs[n : n + 3], refs[n + 3 : 2 * n + 3], refs[2 * n + 3 :])
    total = owners(own_in, place(arrived, groups, halo), ht, s_high, s_low, halo)
    own_out[...] = total
    send_rows(total, h, place(pieces, groups, halo), own, halo)


def forward(own_in, arrived, groups, m_high, m_low, s_high, s_low, out, own, halo):
    high, low = split(own_in[...])
    s_high[0:own, :] = high
    s_low[0:own, :] = low
    collect(place(arrived, groups, halo), s_high, s_low, own, halo)
    for start in range(0, m_high.shape[0], TILE):
        rows = slice(start, start + TILE)
        out(rows, mul_split(m_high[rows, :], m_low[rows, :], s_high[...], s_low[...]))


def fourth_kernel(own_in, *refs, groups, own, halo):
    n = len(groups)
    arrived, (m_high, m_low, h, own_out), pieces, (s_high, s_low) = (
        refs[:n], refs[n : n + 4], refs[n + 4 : 2 * n + 4], refs[2 * n + 4 :])

    def store(rows, block):
        own_out[rows, :] = block

    forward(own_in, arrived, groups, m_high, m_low, s_high, s_low, store, own, halo)
    send_rows(own_out[...], h, place(pieces, groups, halo), own, halo)


def last_kernel(valid, own_in, *refs, groups, own, halo, off, width):
    n = len(groups)
    arrived, (m_high, m_low, out, s_high, s_low, result, sems) = refs[:n], refs[n:]
    copies = []

    def store(rows, block):
        copies.append(write_rows(valid, block, rows, result, out, off, width, sems))

    forward(own_in, arrived, groups, m_high, m_low, s_high, s_low, store, own, halo)
    for copy in copies:
        copy.wait()


def write_rows(valid, block, rows, result, out, off, width, sems):
    ids = lax.broadcasted_iota(jnp.int32, block.shape, 0) + rows.start
    result[rows, :] = jnp.where(ids < valid[0, 0], block, 0.0)
    copy = pltpu.make_async_copy(result.at[rows, :], out.at[0, 0, rows, pl.ds(off, width)], sems.at[rows.start // TILE])
    copy.start()
    return copy


def part_kernel(own_in, *refs, groups, own, halo):
    n = len(groups) - 1
    arrived, (m_high, m_low, out, s_high, s_low) = refs[:n], refs[n:]
    count = len(groups[0]) * halo
    for ref in (s_high, s_low):
        ref[own : own + count, :] = jnp.zeros((count, ref.shape[1]), BF16)

    def store(rows, block):
        out[rows, :] = block

    forward(own_in, arrived, groups[1:], m_high, m_low, s_high, s_low, store, own, halo)


def tail_kernel(valid, part, late, m_high, m_low, so_far, out, result, sems, *, own, off, width):
    del so_far
    high, low = split(late[...])
    cols = slice(own, own + late.shape[0])
    copies = []
    for start in range(0, m_high.shape[0], TILE):
        rows = slice(start, start + TILE)
        block = (mul(m_high[rows, cols], high) + mul(m_high[rows, cols], low)
                 + mul(m_low[rows, cols], high) + part[rows, :])
        copies.append(write_rows(valid, block, rows, result, out, off, width, sems))
    for copy in copies:
        copy.wait()


def body(ctrl, interp_wt, interp_cols, conv_wt, conv_cols, halo_index, valid):
    halo = halo_index.shape[3]
    grid_rows, width_all = ctrl.shape[2:]
    blocks, block_rows = conv_wt.shape[2:4]
    own = blocks * block_rows
    slots = 8 * halo
    ext = own + slots
    far_ctrl, far_wt, far_cols = (
        pltpu.with_memory_space_constraint(array, pltpu.HBM) for array in (ctrl, interp_wt, interp_cols))
    odd = lax.axis_index("ty") % 2
    odd = odd.astype(jnp.int32).reshape(1, 1)
    groups = slot_groups(lax.axis_size("tx"))
    known = dict(groups=groups, own=own, halo=halo)

    def shape(rows, cols, kind=F32):
        return jax.ShapeDtypeStruct((rows, cols), kind)

    def call(kernel, outs, args, specs, scratch=(), aliases=None, out_spec=VMEM, **more):
        return pl.pallas_call(
            functools.partial(kernel, **more),
            out_shape=outs,
            in_specs=list(specs) + [VMEM] * (len(args) - len(specs)),
            out_specs=jax.tree.map(lambda _: out_spec, outs),
            scratch_shapes=list(scratch),
            input_output_aliases=aliases or {},
            compiler_params=PARAMS,
            cost_estimate=pl.CostEstimate(flops=1 << 30, transcendentals=0, bytes_accessed=4 << 20),
        )(*args)

    lanes = 128
    second = (width_all // (2 * lanes)) * lanes
    chunks = [(0, width_all - second), (width_all - second, second)] if second else [(0, width_all)]
    dma = pltpu.SemaphoreType.DMA

    def leaving(width):
        return [shape(own, width)] + [shape(len(group) * halo, width) for group in groups]

    crossing = [group for group in groups if group[0] < CROSSING]
    straight = groups[len(crossing) :]

    def operator(rows):
        return [pltpu.VMEM((rows, grid_rows), BF16)] * 2

    def apart(arrays):
        each = len(arrays) // len(chunks)
        return [list(arrays[k * each : (k + 1) * each]) for k in range(len(chunks))]

    over = [shape(len(group) * halo, width) for _, width in chunks for group in crossing]
    keep = [shape(grid_rows, width_all, BF16)] * 2 + [
        jax.ShapeDtypeStruct(array.shape, array.dtype) for array in (interp_wt, interp_cols)]
    high, low, near_wt, near_cols, *over = call(
        first_kernel, keep + over, (valid, odd, far_ctrl, far_wt, far_cols), [SMEM, SMEM, HBM, HBM, HBM],
        operator(CROSSING * halo) + [pltpu.VMEM(ctrl.shape, F32), dma((3,))],
        chunks=chunks, groups=crossing, own=own, halo=halo)
    rest = []
    for _, width in chunks:
        rest += [shape(own, width)] + [shape(len(group) * halo, width) for group in straight]
    rest = call(rest_kernel, rest, (odd, high, low, near_wt, near_cols), [SMEM],
                operator(ext - CROSSING * halo), chunks=chunks, groups=straight, own=own, halo=halo)
    over, rest = apart(over), apart(rest)
    state = [[mine[0]] + sent + mine[1:] for sent, mine in zip(over, rest)]
    ct_high, ct_low, ht, h = call(
        early_kernel, [shape(ext, own, BF16)] * 2 + [shape(own, slots, BF16), shape(slots, own, BF16)],
        (odd, conv_wt, conv_cols, halo_index), [SMEM], halo=halo)
    c_high, c_low = call(
        late_kernel, [shape(own, ext, BF16)] * 2, (odd, conv_wt, conv_cols), [SMEM], own=own, halo=halo)
    i_high, i_low = call(
        late_kernel, [shape(grid_rows, ext, BF16)] * 2, (odd, interp_wt, interp_cols), [SMEM], own=own, halo=halo)

    def scratch(rows, width):
        return [pltpu.VMEM((rows, width), BF16)] * 2

    def arrive(number, sign):
        mine, *out = state[number]
        return mine, *exchange(out, groups, sign)

    def advance(sign, kernel, operands, rows):
        for number, (_, width) in enumerate(chunks):
            state[number] = call(kernel, leaving(width),
                                 (*arrive(number, sign), *operands), (), scratch(rows, width), **known)

    advance(-1, second_kernel, (ht, ct_high, ct_low), slots)
    advance(-1, third_kernel, (ht, h), slots)
    advance(1, fourth_kernel, (c_high, c_low, h), ext)
    whole = jax.ShapeDtypeStruct(ctrl.shape, F32)
    result = None
    for number, (off, width) in enumerate(chunks):
        mine, *arrived = arrive(number, 1)
        final = [pltpu.VMEM((grid_rows, width), F32), dma((grid_rows // TILE,))]
        if number == 0:
            result = call(last_kernel, whole, (valid, mine, *arrived, i_high, i_low), [SMEM],
                          scratch(ext, width) + final, None, HBM, off=off, width=width, **known)
        else:
            part = call(part_kernel, shape(grid_rows, width), (mine, *arrived[1:], i_high, i_low), (),
                        scratch(ext, width), **known)
            args = (valid, part, arrived[0], i_high, i_low, result)
            result = call(tail_kernel, whole, args, [SMEM] + [VMEM] * 4 + [HBM], final, {5: 0}, HBM,
                          own=own, off=off, width=width)
    return result


def solution(mesh):
    placed = (
        P("ty", "tx", None, None),
        P("ty", "tx", None, None, None),
        P("ty", "tx", None, None),
        P("ty", "tx", None, None, None),
        P("ty", "tx", None, None),
        P("ty", "tx", None, None),
        P("ty", "tx"),
    )

    return jax.shard_map(body, mesh=mesh, in_specs=placed, out_specs=P("ty", "tx", None, None), check_vma=False)
```
